32 devices in a mesh: grp: 2 (over core), dp: 16 (over z, y, x).
Axes of the slice: x: 2, y: 2, z: 4, core: 2. Of those that a mesh axis runs over, the one named last changes fastest.
Arguments:
- version_tags: int32 [32768], P(('grp', 'dp')), may hold values from 0 to 3
- packed_pos: int32 [32768], P(('grp', 'dp')), may hold values from 0 to 32767, as said below
- valid_mask: int32 [32768, 128], P(('grp', 'dp')), may hold values from 0 to 1, as said below
- returns: float32 [32768, 128], P(('grp', 'dp')), may hold values from -16 to 16
- values: float32 [32768, 128], P(('grp', 'dp')), may hold values from -6 to 6
- log_ratio_new: float32 [32768, 128], P(('grp', 'dp')), may hold values from -4 to 4
- log_ratio_prox: float32 [32768, 128], P(('grp', 'dp')), may hold values from -4 to 4
Outputs:
- token_loss: float32 [32768, 128], P(('grp', 'dp'))
- block_loss: float32 [32768], P(('grp', 'dp'))
The draws below stay inside these ranges and needn't reach their ends.
Inputs may be any that keep to these rules, and one draw needn't show every extreme that they name: `packed_pos`: A permutation of the blocks. Blocks stay within their group of 16 devices along dp; each device's 1024 packed positions take 1024 // 16 blocks from every device of its group, those of the s-th device of the group at local packed positions s * (64) onward; which of a device's blocks go where is otherwise arbitrary. `valid_mask`: some blocks have no valid token.
All inputs are finite; a program needn't handle non-finite values.
Results may differ from the reference program's by a relative error of at most 0.00002.
Values sent between devices are 32-bit elements; how exact they have to be, the bound alone decides.
A program may use at most 64 MiB of HBM per device.

```python
import math
import jax
import jax.numpy as jnp
from jax import lax

BLOCK = 128
VERSIONS = 4
BLK_DEV = 1024
BLOCKS = 32768
N_GRP = 2
N_DP = 16


def common_tags(key):
    integer_draws = jax.random.randint(jax.random.fold_in(key, 101), (BLOCKS,), 0, 10)
    return (integer_draws >= 1).astype(jnp.int32) + (integer_draws >= 3).astype(jnp.int32) + (integer_draws >= 6).astype(jnp.int32)


def draw_version_tags(key, part):
    return common_tags(key)


def draw_valid_mask(key, part):
    token_draws = jax.random.randint(jax.random.fold_in(key, 404), (BLOCKS, BLOCK), 0, 4)
    block_draws = jax.random.randint(jax.random.fold_in(key, 405), (BLOCKS,), 0, 32)
    block_index = jnp.arange(BLOCKS, dtype=jnp.int32)
    emptied = jnp.logical_or(block_draws == 0, block_index % 997 == 0)
    keep_block = 1 - emptied.astype(jnp.int32)
    return ((token_draws >= 1).astype(jnp.int32) * keep_block[:, None]).astype(jnp.int32)


def draw_returns(key, part):
    labels = common_tags(key)
    subkeys = jax.random.split(jax.random.fold_in(key, 202), 4)
    onehot = (labels[:, None] == jnp.arange(VERSIONS, dtype=jnp.int32)[None, :]).astype(jnp.float32)
    position = jnp.arange(BLOCKS).astype(jnp.float32) / BLOCKS
    phase_shift = jax.random.uniform(subkeys[3], (), jnp.float32, 0.0, 2.0 * math.pi)
    offsets = jax.random.uniform(subkeys[0], (VERSIONS,), jnp.float32, -2.0, 2.0)
    scales = jnp.exp(jax.random.uniform(subkeys[1], (VERSIONS,), jnp.float32, math.log(0.5), math.log(2.0)))
    jitter = jax.random.truncated_normal(subkeys[2], -6.0, 6.0, (BLOCKS, BLOCK), jnp.float32)
    trend = jnp.sin(6.0 * math.pi * position + phase_shift)
    level = jnp.sum(onehot * offsets[None, :], axis=1) + trend
    spread = jnp.sum(onehot * scales[None, :], axis=1)
    return level[:, None] + spread[:, None] * jitter


def draw_packed_pos(key, part):
    per_peer = BLK_DEV // N_DP
    subkeys = jax.random.split(jax.random.fold_in(key, 303), N_GRP * N_DP)
    orders = jax.vmap(lambda subkey: jax.random.permutation(subkey, BLK_DEV))(subkeys).astype(jnp.int32)
    device = jnp.arange(N_GRP * N_DP, dtype=jnp.int32)[:, None]
    group_index = device // N_DP
    source = device % N_DP
    target = orders // per_peer
    slot_index = orders % per_peer
    packed = group_index * (BLK_DEV * N_DP) + target * BLK_DEV + source * per_peer + slot_index
    return packed.reshape(-1).astype(jnp.int32)


def level_of(own_key, extent, shards, low, high):
    def one(dim, shards_of):
        draws = jax.random.uniform(jax.random.fold_in(jax.random.fold_in(own_key, 6), dim), (shards_of,), jnp.float32, low / len(shards), high / len(shards))
        return jnp.repeat(jnp.exp(draws), extent[dim] // shards_of).reshape((-1,) + (1,) * (len(extent) - dim - 1))

    level = one(*shards[0])
    for cut in shards[1:]:
        level = level * one(*cut)
    return level


def bell_draw(own_key, extent, scale, reach, shards=(), held_as=jnp.bfloat16):
    array = jax.random.normal(own_key, extent, jnp.float32) * scale
    if len(shards) > 0:
        array = level_of(own_key, extent, shards, -0.22, 0.18) * array
    return jnp.clip(array, min=-reach, max=reach).astype(held_as)


def setup_inputs(seed: int = 0) -> dict:
    arg_keys = jax.random.split(jax.random.key(seed), 8)
    version_tags = draw_version_tags(jax.random.fold_in(arg_keys[7], 71), 0)
    packed_pos = draw_packed_pos(jax.random.fold_in(arg_keys[7], 71), 0)
    valid_mask = draw_valid_mask(jax.random.fold_in(arg_keys[7], 71), 0)
    returns = draw_returns(jax.random.fold_in(arg_keys[7], 71), 0)
    values = bell_draw(arg_keys[4], (BLOCKS, BLOCK), 1.0, 6.0, ((0, 32),), jnp.float32)
    log_ratio_new = bell_draw(arg_keys[5], (BLOCKS, BLOCK), 0.25, 4.0, ((0, 32),), jnp.float32)
    log_ratio_prox = bell_draw(arg_keys[6], (BLOCKS, BLOCK), 0.25, 4.0, ((0, 32),), jnp.float32)
    return dict(version_tags=version_tags, packed_pos=packed_pos, valid_mask=valid_mask, returns=returns, values=values, log_ratio_new=log_ratio_new, log_ratio_prox=log_ratio_prox)


def reference(version_tags, packed_pos, valid_mask, returns, values, log_ratio_new, log_ratio_prox):
    advantage = returns - values
    maskf = valid_mask.astype(jnp.float32)
    onehot = (version_tags[:, None] == jnp.arange(VERSIONS, dtype=jnp.int32)[None, :]).astype(jnp.float32)
    block_count = lax.optimization_barrier(jnp.sum(maskf, axis=1))
    counts = lax.optimization_barrier(jnp.sum(onehot * block_count[:, None], axis=0))
    adv_sums = lax.optimization_barrier(jnp.sum(onehot * lax.optimization_barrier(jnp.sum(maskf * advantage, axis=1))[:, None], axis=0))
    version_mean = adv_sums / jnp.maximum(counts, 1.0)
    block_mean = lax.optimization_barrier(jnp.sum(onehot * version_mean[None, :], axis=1))
    centered = advantage - block_mean[:, None]
    squares = lax.optimization_barrier(jnp.sum(onehot * lax.optimization_barrier(jnp.sum(maskf * centered * centered, axis=1))[:, None], axis=0))
    version_scale = 1.0 / jnp.sqrt(squares / jnp.maximum(counts, 1.0) + 0.05)
    white = centered * lax.optimization_barrier(jnp.sum(onehot * version_scale[None, :], axis=1))[:, None]
    prob_ratio = jnp.exp(log_ratio_new)
    weight = maskf * jnp.exp(log_ratio_prox)
    clipped = jnp.clip(prob_ratio, 0.8, 1.2)
    loss = -weight * jnp.minimum(prob_ratio * white, clipped * white)
    per_block = lax.optimization_barrier(jnp.sum(loss, axis=1)) / jnp.maximum(block_count, 1.0)
    token_loss = jnp.zeros_like(loss).at[packed_pos].set(loss)
    block_loss = jnp.zeros_like(per_block).at[packed_pos].set(per_block)
    return (token_loss, block_loss)
```

```python
import functools

import jax
import jax.numpy as jnp
from jax import lax
from jax.experimental import pallas as pl
from jax.experimental.pallas import tpu as pltpu
from jax.sharding import PartitionSpec as P

VERSIONS = 4
LANES = 128
F32 = jnp.float32
BF16 = jnp.bfloat16
MESH = pl.DeviceIdType.MESH
NT = (((1,), (1,)), ((), ()))


def fold(array):
    return jnp.sum(array.reshape(-1, 8, array.shape[-1]), axis=0)


def total(array):
    return jnp.sum(jnp.sum(array, axis=0, keepdims=True), axis=1, keepdims=True)


def pick(tags, per_version):
    chosen = per_version[-1]
    for v in range(VERSIONS - 2, -1, -1):
        chosen = jnp.where(tags == v, per_version[v], chosen)
    return chosen


def kernel(
    n_grp, n_dp,
    tags_ref, packed_ref, mask_hbm, ret_hbm, val_hbm, new_hbm, prox_hbm,
    tok_out, blk_out,
    mask_s, ret_s, val_s, new_s, prox_s, tags_s, perm_s, split_s, send_s, bsend_s, stats_s,
    load_sem, st_send, st_recv, tok_send, tok_recv, blk_send, blk_recv, own_sem,
):
    n_all = n_grp * n_dp
    my_grp, my_dp = lax.axis_index("grp"), lax.axis_index("dp")
    me = my_grp * n_dp + my_dp
    rows = ret_s.shape[0]
    tiles = rows // LANES
    per_peer = rows // n_dp
    group = max(1, 256 // per_peer)
    chunk = group * per_peer
    n_chunks = rows // chunk

    def device(index):
        return {"grp": index // n_dp, "dp": lax.rem(index, n_dp)}

    loads = [
        pltpu.make_async_copy(src, dst, load_sem.at[i])
        for i, (src, dst) in enumerate(
            ((ret_hbm, ret_s), (val_hbm, val_s), (mask_hbm, mask_s), (new_hbm, new_s), (prox_hbm, prox_s))
        )
    ]
    for load in loads:
        load.start()

    barrier = pltpu.get_barrier_semaphore()

    @pl.loop(1, n_all)
    def _(k):
        pl.semaphore_signal(
            barrier, inc=1, device_id=device(lax.rem(me + k, n_all)), device_id_type=MESH
        )

    eye = lax.broadcasted_iota(jnp.int32, (LANES, LANES), 0) == lax.broadcasted_iota(
        jnp.int32, (LANES, LANES), 1
    )
    ones = jnp.ones((LANES, LANES), BF16)
    for t in range(tiles):
        row = tags_ref[t : t + 1, :].astype(F32)
        spread = jnp.where(eye, jnp.broadcast_to(row, (LANES, LANES)), 0.0).astype(BF16)
        tags_s[t * LANES : (t + 1) * LANES, :] = jnp.dot(spread, ones, preferred_element_type=F32)

    for load in loads[:3]:
        load.wait()
    counts = [jnp.zeros((8, LANES), F32)] * VERSIONS
    sums = [jnp.zeros((8, LANES), F32)] * VERSIONS
    for t in range(tiles):
        at = slice(t * LANES, (t + 1) * LANES)
        maskf = mask_s[at, :].astype(F32)
        advantage = ret_s[at, :] - val_s[at, :]
        ret_s[at, :] = advantage
        tags = tags_s[at, :]
        for v in range(VERSIONS):
            valid = jnp.where(tags == v, maskf, 0.0)
            counts[v] = counts[v] + fold(valid)
            sums[v] = sums[v] + fold(valid * advantage)
    counts = [total(c) for c in counts]
    means = [total(s) / jnp.maximum(c, 1.0) for s, c in zip(sums, counts)]
    squares = [jnp.zeros((8, LANES), F32)] * VERSIONS
    for t in range(tiles):
        at = slice(t * LANES, (t + 1) * LANES)
        tags = tags_s[at, :]
        centered = ret_s[at, :] - pick(tags, means)
        square = mask_s[at, :].astype(F32) * centered * centered
        for v in range(VERSIONS):
            squares[v] = squares[v] + fold(jnp.where(tags == v, square, 0.0))
    squares = [total(s) for s in squares]
    lane = lax.broadcasted_iota(jnp.int32, (1, LANES), 1)
    message = jnp.zeros((1, LANES), F32)
    for i, value in enumerate(counts + means + squares):
        message = jnp.where(lane == i, value, message)
    stats_s[me] = message

    pl.semaphore_wait(barrier, n_all - 1)

    @pl.loop(1, n_all)
    def _(k):
        pltpu.make_async_remote_copy(
            src_ref=stats_s.at[me], dst_ref=stats_s.at[me], send_sem=st_send, recv_sem=st_recv,
            device_id=device(lax.rem(me + k, n_all)), device_id_type=MESH,
        ).start()

    base = my_grp * (rows * n_dp) + my_dp * per_peer
    for c in range(n_chunks):
        slot = lax.broadcasted_iota(jnp.int32, (chunk, LANES), 0)
        want = base + (slot // per_peer + c * group) * rows + lax.rem(slot, per_peer)
        for t in range(tiles):
            hit = want == packed_ref[t : t + 1, :]
            perm_s[c * chunk : (c + 1) * chunk, t * LANES : (t + 1) * LANES] = (
                jnp.where(hit, 1.0, 0.0).astype(BF16)
            )
    for load in loads[3:]:
        load.wait()
    block_counts = []
    for t in range(tiles):
        at = slice(t * LANES, (t + 1) * LANES)
        maskf = mask_s[at, :].astype(F32)
        weight = -maskf * jnp.exp(prox_s[at, :])
        ratio = jnp.exp(new_s[at, :])
        new_s[at, :] = weight * ratio
        prox_s[at, :] = weight * jnp.clip(ratio, 0.8, 1.2)
        block_counts.append(
            lax.dot_general(ones[:8], maskf.astype(BF16), NT, preferred_element_type=F32)
        )

    everyone = stats_s.at[pl.ds(0, n_all - 1)]
    pltpu.make_async_copy(everyone, everyone, st_recv).wait()
    every_count = stats_s[...]
    every_mean = pltpu.roll(every_count, LANES - VERSIONS, 2)
    every_square = pltpu.roll(every_count, LANES - 2 * VERSIONS, 2)
    total_count = jnp.maximum(jnp.sum(every_count, axis=0), 1.0)
    mean_row = jnp.sum(every_count * every_mean, axis=0) / total_count
    off = every_mean - mean_row[None]
    square_row = jnp.sum(every_square + every_count * off * off, axis=0)
    scale_row = 1.0 / jnp.sqrt(square_row / total_count + 0.05)
    means = [mean_row[:, v : v + 1] for v in range(VERSIONS)]
    scales = [scale_row[:, v : v + 1] for v in range(VERSIONS)]

    for t in range(tiles):
        at = slice(t * LANES, (t + 1) * LANES)
        tags = tags_s[at, :]
        white = (ret_s[at, :] - pick(tags, means)) * pick(tags, scales)
        loss = jnp.maximum(new_s[at, :] * white, prox_s[at, :] * white)
        high = loss.astype(BF16)
        split_s[at, :LANES] = high
        split_s[at, LANES:] = (loss - high.astype(F32)).astype(BF16)

    my_chunk = my_dp // group
    for i in range(n_chunks):
        c = lax.rem(my_chunk + i, n_chunks)
        at = pl.ds(pl.multiple_of(c * chunk, chunk), chunk)
        parts = jnp.dot(perm_s[at, :], split_s[...], preferred_element_type=F32)
        send_s[at, :] = parts[:, :LANES] + parts[:, LANES:]
        for q in range(group):
            peer = c * group + q
            src = send_s.at[pl.ds(pl.multiple_of(peer * per_peer, per_peer), per_peer)]
            dst = tok_out.at[pl.ds(pl.multiple_of(my_dp * per_peer, per_peer), per_peer)]

            @pl.when(peer != my_dp)
            def _():
                pltpu.make_async_remote_copy(
                    src_ref=src, dst_ref=dst, send_sem=tok_send, recv_sem=tok_recv,
                    device_id={"grp": my_grp, "dp": peer}, device_id_type=MESH,
                ).start()

            @pl.when(peer == my_dp)
            def _():
                pltpu.make_async_copy(src, dst, own_sem).start()

    sub = lax.broadcasted_iota(jnp.int32, (8, LANES), 0)
    pieces = []
    for t in range(tiles):
        at = slice(t * LANES, (t + 1) * LANES)
        block = lax.dot_general(
            jnp.ones((8, 2 * LANES), BF16), split_s[at, :], NT, preferred_element_type=F32
        ) / jnp.maximum(block_counts[t], 1.0)
        high = block.astype(BF16).astype(F32)
        middle = (block - high).astype(BF16).astype(F32)
        low = block - high - middle
        piece = jnp.where(sub == 0, high, jnp.where(sub == 1, middle, jnp.where(sub == 2, low, 0.0)))
        pieces.append(piece.astype(BF16))
    blocks = jnp.concatenate(pieces, axis=1)
    for i in range(n_chunks):
        c = lax.rem(my_chunk + i, n_chunks)
        at = pl.ds(pl.multiple_of(c * chunk, chunk), chunk)
        moved = jnp.sum(
            lax.dot_general(blocks, perm_s[at, :], NT, preferred_element_type=F32), axis=0, keepdims=True
        )
        for q in range(group):
            peer = c * group + q
            part = moved[:, q * per_peer : (q + 1) * per_peer]
            bsend_s[peer] = part

            @pl.when(peer != my_dp)
            def _():
                pltpu.make_async_remote_copy(
                    src_ref=bsend_s.at[peer], dst_ref=blk_out.at[my_dp], send_sem=blk_send,
                    recv_sem=blk_recv, device_id={"grp": my_grp, "dp": peer}, device_id_type=MESH,
                ).start()

            @pl.when(peer == my_dp)
            def _():
                blk_out[my_dp] = part

    own = send_s.at[pl.ds(0, per_peer)]
    pltpu.make_async_copy(own, tok_out.at[pl.ds(0, per_peer)], own_sem).wait()
    pltpu.make_async_copy(everyone, everyone, st_send).wait()
    others = pl.ds(0, rows - per_peer)
    for sem in (tok_send, tok_recv):
        pltpu.make_async_copy(send_s.at[others], tok_out.at[others], sem).wait()
    peers = bsend_s.at[pl.ds(0, n_dp - 1)]
    for sem in (blk_send, blk_recv):
        pltpu.make_async_copy(peers, peers, sem).wait()


def solution(mesh):
    n_grp, n_dp = mesh.shape["grp"], mesh.shape["dp"]

    def on_device(version_tags, packed_pos, valid_mask, returns, values, log_ratio_new, log_ratio_prox):
        rows, width = returns.shape
        n_all = n_grp * n_dp
        per_peer = rows // n_dp
        vmem = pl.BlockSpec(memory_space=pltpu.VMEM)
        anywhere = pl.BlockSpec(memory_space=pl.ANY)
        dma = pltpu.SemaphoreType.DMA
        full = pltpu.VMEM((rows, width), F32)
        token_loss, block_loss = pl.pallas_call(
            functools.partial(kernel, n_grp, n_dp),
            out_shape=(
                jax.ShapeDtypeStruct((rows, width), F32),
                jax.ShapeDtypeStruct((n_dp, 1, per_peer), F32),
            ),
            in_specs=[vmem, vmem] + [anywhere] * 5,
            out_specs=(anywhere, vmem),
            scratch_shapes=[
                pltpu.VMEM((rows, width), jnp.int32), full, full, full, full, full,
                pltpu.VMEM((rows, rows), BF16),
                pltpu.VMEM((rows, 2 * width), BF16),
                full,
                pltpu.VMEM((n_dp, 1, per_peer), F32),
                pltpu.VMEM((n_all, 1, width), F32),
                dma((5,)), dma, dma, dma, dma, dma, dma, dma,
            ],
            compiler_params=pltpu.CompilerParams(collective_id=0, has_side_effects=True),
        )(
            version_tags.reshape(rows // LANES, LANES), packed_pos.reshape(rows // LANES, LANES),
            valid_mask, returns, values, log_ratio_new, log_ratio_prox,
        )
        return token_loss, block_loss.reshape(rows)

    each = P(("grp", "dp"))
    wide = P(("grp", "dp"), None)
    return jax.shard_map(
        on_device, mesh=mesh, in_specs=(each, each) + (wide,) * 5, out_specs=(wide, each), check_vma=False
    )
```

```python
import functools

import jax
import jax.numpy as jnp
from jax import lax
from jax.experimental import pallas as pl
from jax.experimental.pallas import tpu as pltpu
from jax.sharding import PartitionSpec as P

VERSIONS = 4
LANES = 128
F32 = jnp.float32
BF16 = jnp.bfloat16
MESH = pl.DeviceIdType.MESH
NT = (((1,), (1,)), ((), ()))


def fold(array):
    return jnp.sum(array.reshape(-1, 8, array.shape[-1]), axis=0)


def total(array):
    return jnp.sum(jnp.sum(array, axis=0, keepdims=True), axis=1, keepdims=True)


def pick(tags, per_version):
    chosen = per_version[-1]
    for v in range(VERSIONS - 2, -1, -1):
        chosen = jnp.where(tags == v, per_version[v], chosen)
    return chosen


def kernel(
    n_grp, n_dp,
    tags_ref, packed_ref, mask_hbm, ret_hbm, val_hbm, new_hbm, prox_hbm,
    tok_out, blk_out,
    mask_s, ret_s, val_s, new_s, prox_s, tags_s, perm_s, split_s, send_s, bsend_s, brecv_s, stats_s,
    load_sem, st_send, st_recv, tok_send, tok_recv, blk_send, blk_recv, own_sem,
):
    n_all = n_grp * n_dp
    my_grp, my_dp = lax.axis_index("grp"), lax.axis_index("dp")
    me = my_grp * n_dp + my_dp
    rows = ret_s.shape[0]
    tiles = rows // LANES
    per_peer = rows // n_dp
    group = max(1, 256 // per_peer)
    chunk = group * per_peer
    n_chunks = rows // chunk

    def device(index):
        return {"grp": index // n_dp, "dp": lax.rem(index, n_dp)}

    loads = [
        pltpu.make_async_copy(src, dst, load_sem.at[i])
        for i, (src, dst) in enumerate(
            ((ret_hbm, ret_s), (val_hbm, val_s), (mask_hbm, mask_s), (new_hbm, new_s), (prox_hbm, prox_s))
        )
    ]
    for load in loads:
        load.start()

    barrier = pltpu.get_barrier_semaphore()

    @pl.loop(1, n_all)
    def _(k):
        pl.semaphore_signal(
            barrier, inc=1, device_id=device(lax.rem(me + k, n_all)), device_id_type=MESH
        )

    eye = lax.broadcasted_iota(jnp.int32, (LANES, LANES), 0) == lax.broadcasted_iota(
        jnp.int32, (LANES, LANES), 1
    )
    ones = jnp.ones((LANES, LANES), BF16)
    for t in range(tiles):
        row = tags_ref[t : t + 1, :].astype(F32)
        spread = jnp.where(eye, jnp.broadcast_to(row, (LANES, LANES)), 0.0).astype(BF16)
        tags_s[t * LANES : (t + 1) * LANES, :] = jnp.dot(spread, ones, preferred_element_type=F32)

    for load in loads[:3]:
        load.wait()
    counts = [jnp.zeros((8, LANES), F32)] * VERSIONS
    sums = [jnp.zeros((8, LANES), F32)] * VERSIONS
    for t in range(tiles):
        at = slice(t * LANES, (t + 1) * LANES)
        maskf = mask_s[at, :].astype(F32)
        advantage = ret_s[at, :] - val_s[at, :]
        ret_s[at, :] = advantage
        tags = tags_s[at, :]
        for v in range(VERSIONS):
            valid = jnp.where(tags == v, maskf, 0.0)
            counts[v] = counts[v] + fold(valid)
            sums[v] = sums[v] + fold(valid * advantage)
    counts = [total(c) for c in counts]
    means = [total(s) / jnp.maximum(c, 1.0) for s, c in zip(sums, counts)]
    squares = [jnp.zeros((8, LANES), F32)] * VERSIONS
    for t in range(tiles):
        at = slice(t * LANES, (t + 1) * LANES)
        tags = tags_s[at, :]
        centered = ret_s[at, :] - pick(tags, means)
        square = mask_s[at, :].astype(F32) * centered * centered
        for v in range(VERSIONS):
            squares[v] = squares[v] + fold(jnp.where(tags == v, square, 0.0))
    squares = [total(s) for s in squares]
    lane = lax.broadcasted_iota(jnp.int32, (1, LANES), 1)
    message = jnp.zeros((1, LANES), F32)
    for i, value in enumerate(counts + means + squares):
        message = jnp.where(lane == i, value, message)
    stats_s[me] = message

    pl.semaphore_wait(barrier, n_all - 1)

    @pl.loop(1, n_all)
    def _(k):
        pltpu.make_async_remote_copy(
            src_ref=stats_s.at[me], dst_ref=stats_s.at[me], send_sem=st_send, recv_sem=st_recv,
            device_id=device(lax.rem(me + k, n_all)), device_id_type=MESH,
        ).start()

    base = my_grp * (rows * n_dp) + my_dp * per_peer
    for c in range(n_chunks):
        slot = lax.broadcasted_iota(jnp.int32, (chunk, LANES), 0)
        want = base + (slot // per_peer + c * group) * rows + lax.rem(slot, per_peer)
        for t in range(tiles):
            hit = want == packed_ref[t : t + 1, :]
            perm_s[c * chunk : (c + 1) * chunk, t * LANES : (t + 1) * LANES] = (
                jnp.where(hit, 1.0, 0.0).astype(BF16)
            )
    for load in loads[3:]:
        load.wait()
    block_counts = []
    for t in range(tiles):
        at = slice(t * LANES, (t + 1) * LANES)
        maskf = mask_s[at, :].astype(F32)
        weight = -maskf * jnp.exp(prox_s[at, :])
        ratio = jnp.exp(new_s[at, :])
        new_s[at, :] = weight * ratio
        prox_s[at, :] = weight * jnp.clip(ratio, 0.8, 1.2)
        block_counts.append(
            lax.dot_general(ones[:8], maskf.astype(BF16), NT, preferred_element_type=F32)
        )

    everyone = stats_s.at[pl.ds(0, n_all - 1)]
    pltpu.make_async_copy(everyone, everyone, st_recv).wait()
    every_count = stats_s[...]
    every_mean = pltpu.roll(every_count, LANES - VERSIONS, 2)
    every_square = pltpu.roll(every_count, LANES - 2 * VERSIONS, 2)
    total_count = jnp.maximum(jnp.sum(every_count, axis=0), 1.0)
    mean_row = jnp.sum(every_count * every_mean, axis=0) / total_count
    off = every_mean - mean_row[None]
    square_row = jnp.sum(every_square + every_count * off * off, axis=0)
    scale_row = 1.0 / jnp.sqrt(square_row / total_count + 0.05)
    means = [mean_row[:, v : v + 1] for v in range(VERSIONS)]
    scales = [scale_row[:, v : v + 1] for v in range(VERSIONS)]

    for t in range(tiles):
        at = slice(t * LANES, (t + 1) * LANES)
        tags = tags_s[at, :]
        white = (ret_s[at, :] - pick(tags, means)) * pick(tags, scales)
        loss = jnp.maximum(new_s[at, :] * white, prox_s[at, :] * white)
        high = loss.astype(BF16)
        split_s[at, :LANES] = high
        split_s[at, LANES:] = (loss - high.astype(F32)).astype(BF16)

    my_chunk = my_dp // group
    for i in range(n_chunks):
        c = lax.rem(my_chunk + i, n_chunks)
        at = pl.ds(pl.multiple_of(c * chunk, chunk), chunk)
        parts = jnp.dot(perm_s[at, :], split_s[...], preferred_element_type=F32)
        send_s[at, :] = parts[:, :LANES] + parts[:, LANES:]
        for q in range(group):
            peer = c * group + q
            src = send_s.at[pl.ds(pl.multiple_of(peer * per_peer, per_peer), per_peer)]
            dst = tok_out.at[pl.ds(pl.multiple_of(my_dp * per_peer, per_peer), per_peer)]

            @pl.when(peer != my_dp)
            def _():
                pltpu.make_async_remote_copy(
                    src_ref=src, dst_ref=dst, send_sem=tok_send, recv_sem=tok_recv,
                    device_id={"grp": my_grp, "dp": peer}, device_id_type=MESH,
                ).start()

            @pl.when(peer == my_dp)
            def _():
                pltpu.make_async_copy(src, dst, own_sem).start()

    sub = lax.broadcasted_iota(jnp.int32, (8, LANES), 0)
    pieces = []
    for t in range(tiles):
        at = slice(t * LANES, (t + 1) * LANES)
        block = lax.dot_general(
            jnp.ones((8, 2 * LANES), BF16), split_s[at, :], NT, preferred_element_type=F32
        ) / jnp.maximum(block_counts[t], 1.0)
        high = block.astype(BF16).astype(F32)
        middle = (block - high).astype(BF16).astype(F32)
        low = block - high - middle
        piece = jnp.where(sub == 0, high, jnp.where(sub == 1, middle, jnp.where(sub == 2, low, 0.0)))
        pieces.append(piece.astype(BF16))
    blocks = jnp.concatenate(pieces, axis=1)
    for i in range(n_chunks):
        c = lax.rem(my_chunk + i, n_chunks)
        at = pl.ds(pl.multiple_of(c * chunk, chunk), chunk)
        moved = jnp.sum(
            lax.dot_general(blocks, perm_s[at, :], NT, preferred_element_type=F32), axis=0, keepdims=True
        )
        for q in range(group):
            peer = c * group + q
            part = moved[:, q * per_peer : (q + 1) * per_peer]
            bsend_s[peer] = jnp.concatenate(
                [part, jnp.zeros((1, LANES - per_peer), F32)], axis=1
            )

            @pl.when(peer != my_dp)
            def _():
                pltpu.make_async_remote_copy(
                    src_ref=bsend_s.at[peer], dst_ref=brecv_s.at[my_dp], send_sem=blk_send,
                    recv_sem=blk_recv, device_id={"grp": my_grp, "dp": peer}, device_id_type=MESH,
                ).start()

            @pl.when(peer == my_dp)
            def _():
                brecv_s[my_dp] = bsend_s[peer]

    own = send_s.at[pl.ds(0, per_peer)]
    pltpu.make_async_copy(own, tok_out.at[pl.ds(0, per_peer)], own_sem).wait()
    pltpu.make_async_copy(everyone, everyone, st_send).wait()
    others = pl.ds(0, rows - per_peer)
    for sem in (tok_send, tok_recv):
        pltpu.make_async_copy(send_s.at[others], tok_out.at[others], sem).wait()
    peers = bsend_s.at[pl.ds(0, n_dp - 1)]
    for sem in (blk_send, blk_recv):
        pltpu.make_async_copy(peers, peers, sem).wait()
    beside = LANES // per_peer
    for r in range(tiles):
        line = brecv_s[r * beside]
        for q in range(1, beside):
            line = line + pltpu.roll(brecv_s[r * beside + q], q * per_peer, 1)
        blk_out[r : r + 1, :] = line


def solution(mesh):
    n_grp, n_dp = mesh.shape["grp"], mesh.shape["dp"]

    def on_device(version_tags, packed_pos, valid_mask, returns, values, log_ratio_new, log_ratio_prox):
        rows, width = returns.shape
        n_all = n_grp * n_dp
        per_peer = rows // n_dp
        vmem = pl.BlockSpec(memory_space=pltpu.VMEM)
        anywhere = pl.BlockSpec(memory_space=pl.ANY)
        dma = pltpu.SemaphoreType.DMA
        full = pltpu.VMEM((rows, width), F32)
        token_loss, block_loss = pl.pallas_call(
            functools.partial(kernel, n_grp, n_dp),
            out_shape=(
                pltpu.VMEM((rows, width), F32),
                pltpu.VMEM((rows // LANES, LANES), F32),
            ),
            in_specs=[vmem, vmem] + [anywhere] * 5,
            out_specs=(vmem, vmem),
            scratch_shapes=[
                pltpu.VMEM((rows, width), jnp.int32), full, full, full, full, full,
                pltpu.VMEM((rows, rows), BF16),
                pltpu.VMEM((rows, 2 * width), BF16),
                full,
                pltpu.VMEM((n_dp, 1, width), F32),
                pltpu.VMEM((n_dp, 1, width), F32),
                pltpu.VMEM((n_all, 1, width), F32),
                dma((5,)), dma, dma, dma, dma, dma, dma, dma,
            ],
            compiler_params=pltpu.CompilerParams(collective_id=0, has_side_effects=True),
        )(
            version_tags.reshape(rows // LANES, LANES), packed_pos.reshape(rows // LANES, LANES),
            valid_mask, returns, values, log_ratio_new, log_ratio_prox,
        )
        return token_loss, block_loss.reshape(rows)

    each = P(("grp", "dp"))
    wide = P(("grp", "dp"), None)
    return jax.shard_map(
        on_device, mesh=mesh, in_specs=(each, each) + (wide,) * 5, out_specs=(wide, each), check_vma=False
    )
```

```python
import functools

import jax
import jax.numpy as jnp
from jax import lax
from jax.experimental import pallas as pl
from jax.experimental.pallas import tpu as pltpu
from jax.sharding import PartitionSpec as P

VERSIONS = 4
LANES = 128
F32 = jnp.float32
BF16 = jnp.bfloat16
MESH = pl.DeviceIdType.MESH
NT = (((1,), (1,)), ((), ()))


def fold(array):
    return jnp.sum(array.reshape(-1, 8, array.shape[-1]), axis=0)


def total(array):
    return jnp.sum(jnp.sum(array, axis=0, keepdims=True), axis=1, keepdims=True)


def pick(tags, per_version):
    chosen = per_version[-1]
    for v in range(VERSIONS - 2, -1, -1):
        chosen = jnp.where(tags == v, per_version[v], chosen)
    return chosen


def kernel(
    n_grp, n_dp,
    tags_ref, packed_ref, mask_hbm, ret_hbm, val_hbm, new_hbm, prox_hbm,
    tok_out, blk_out,
    mask_s, ret_s, val_s, new_s, prox_s, tags_s, perm_s, split_s, send_s, bsend_s, brecv_s, stats_s,
    load_sem, st_send, st_recv, tok_send, tok_recv, blk_send, blk_recv, own_sem,
):
    n_all = n_grp * n_dp
    my_grp, my_dp = lax.axis_index("grp"), lax.axis_index("dp")
    me = my_grp * n_dp + my_dp
    rows = ret_s.shape[0]
    tiles = rows // LANES
    per_peer = rows // n_dp
    group = max(1, 256 // per_peer)
    chunk = group * per_peer
    n_chunks = rows // chunk

    def device(index):
        return {"grp": index // n_dp, "dp": lax.rem(index, n_dp)}

    loads = [
        pltpu.make_async_copy(src, dst, load_sem.at[i])
        for i, (src, dst) in enumerate(
            ((ret_hbm, ret_s), (val_hbm, val_s), (mask_hbm, mask_s), (new_hbm, new_s), (prox_hbm, prox_s))
        )
    ]
    for load in loads:
        load.start()

    barrier = pltpu.get_barrier_semaphore()

    @pl.loop(1, n_all, unroll=n_all <= 64)
    def _(k):
        pl.semaphore_signal(
            barrier, inc=1, device_id=device(lax.rem(me + k, n_all)), device_id_type=MESH
        )

    eye = lax.broadcasted_iota(jnp.int32, (LANES, LANES), 0) == lax.broadcasted_iota(
        jnp.int32, (LANES, LANES), 1
    )
    ones = jnp.ones((LANES, LANES), BF16)
    for t in range(tiles):
        row = tags_ref[t : t + 1, :].astype(F32)
        spread = jnp.where(eye, jnp.broadcast_to(row, (LANES, LANES)), 0.0).astype(BF16)
        tags_s[t * LANES : (t + 1) * LANES, :] = jnp.dot(spread, ones, preferred_element_type=F32)

    for load in loads[:3]:
        load.wait()
    counts = [jnp.zeros((8, LANES), F32)] * VERSIONS
    sums = [jnp.zeros((8, LANES), F32)] * VERSIONS
    for t in range(tiles):
        at = slice(t * LANES, (t + 1) * LANES)
        maskf = mask_s[at, :].astype(F32)
        advantage = ret_s[at, :] - val_s[at, :]
        ret_s[at, :] = advantage
        tags = tags_s[at, :]
        for v in range(VERSIONS):
            valid = jnp.where(tags == v, maskf, 0.0)
            counts[v] = counts[v] + fold(valid)
            sums[v] = sums[v] + fold(valid * advantage)
    counts = [total(c) for c in counts]
    means = [total(s) / jnp.maximum(c, 1.0) for s, c in zip(sums, counts)]
    squares = [jnp.zeros((8, LANES), F32)] * VERSIONS
    for t in range(tiles):
        at = slice(t * LANES, (t + 1) * LANES)
        tags = tags_s[at, :]
        centered = ret_s[at, :] - pick(tags, means)
        square = mask_s[at, :].astype(F32) * centered * centered
        for v in range(VERSIONS):
            squares[v] = squares[v] + fold(jnp.where(tags == v, square, 0.0))
    squares = [total(s) for s in squares]
    lane = lax.broadcasted_iota(jnp.int32, (1, LANES), 1)
    message = jnp.zeros((1, LANES), F32)
    for i, value in enumerate(counts + means + squares):
        message = jnp.where(lane == i, value, message)
    stats_s[me] = message

    pl.semaphore_wait(barrier, n_all - 1)

    @pl.loop(1, n_all, unroll=n_all <= 64)
    def _(k):
        pltpu.make_async_remote_copy(
            src_ref=stats_s.at[me], dst_ref=stats_s.at[me], send_sem=st_send, recv_sem=st_recv,
            device_id=device(lax.rem(me + k, n_all)), device_id_type=MESH,
        ).start()

    base = my_grp * (rows * n_dp) + my_dp * per_peer
    for c in range(n_chunks):
        slot = lax.broadcasted_iota(jnp.int32, (chunk, LANES), 0)
        want = base + (slot // per_peer + c * group) * rows + lax.rem(slot, per_peer)
        for t in range(tiles):
            hit = want == packed_ref[t : t + 1, :]
            perm_s[c * chunk : (c + 1) * chunk, t * LANES : (t + 1) * LANES] = (
                jnp.where(hit, 1.0, 0.0).astype(BF16)
            )
    for load in loads[3:]:
        load.wait()
    block_counts = []
    for t in range(tiles):
        at = slice(t * LANES, (t + 1) * LANES)
        maskf = mask_s[at, :].astype(F32)
        weight = -maskf * jnp.exp(prox_s[at, :])
        ratio = jnp.exp(new_s[at, :])
        new_s[at, :] = weight * ratio
        prox_s[at, :] = weight * jnp.clip(ratio, 0.8, 1.2)
        block_counts.append(
            lax.dot_general(ones[:8], maskf.astype(BF16), NT, preferred_element_type=F32)
        )

    everyone = stats_s.at[pl.ds(0, n_all - 1)]
    pltpu.make_async_copy(everyone, everyone, st_recv).wait()
    every_count = stats_s[...]
    every_mean = pltpu.roll(every_count, LANES - VERSIONS, 2)
    every_square = pltpu.roll(every_count, LANES - 2 * VERSIONS, 2)
    total_count = jnp.maximum(jnp.sum(every_count, axis=0), 1.0)
    mean_row = jnp.sum(every_count * every_mean, axis=0) / total_count
    off = every_mean - mean_row[None]
    square_row = jnp.sum(every_square + every_count * off * off, axis=0)
    scale_row = 1.0 / jnp.sqrt(square_row / total_count + 0.05)
    means = [mean_row[:, v : v + 1] for v in range(VERSIONS)]
    scales = [scale_row[:, v : v + 1] for v in range(VERSIONS)]

    for t in range(tiles):
        at = slice(t * LANES, (t + 1) * LANES)
        tags = tags_s[at, :]
        white = (ret_s[at, :] - pick(tags, means)) * pick(tags, scales)
        loss = jnp.maximum(new_s[at, :] * white, prox_s[at, :] * white)
        high = loss.astype(BF16)
        split_s[at, :LANES] = high
        split_s[at, LANES:] = (loss - high.astype(F32)).astype(BF16)

    my_chunk = my_dp // group
    for i in range(n_chunks):
        c = jnp.where(my_chunk < n_chunks // 2, n_chunks - 1 - i, i)
        at = pl.ds(pl.multiple_of(c * chunk, chunk), chunk)
        parts = jnp.dot(perm_s[at, :], split_s[...], preferred_element_type=F32)
        send_s[at, :] = parts[:, :LANES] + parts[:, LANES:]
        for q in range(group):
            peer = c * group + q
            src = send_s.at[pl.ds(pl.multiple_of(peer * per_peer, per_peer), per_peer)]
            dst = tok_out.at[pl.ds(pl.multiple_of(my_dp * per_peer, per_peer), per_peer)]

            @pl.when(peer != my_dp)
            def _():
                pltpu.make_async_remote_copy(
                    src_ref=src, dst_ref=dst, send_sem=tok_send, recv_sem=tok_recv,
                    device_id={"grp": my_grp, "dp": peer}, device_id_type=MESH,
                ).start()

            @pl.when(peer == my_dp)
            def _():
                pltpu.make_async_copy(src, dst, own_sem).start()

    sub = lax.broadcasted_iota(jnp.int32, (8, LANES), 0)
    pieces = []
    for t in range(tiles):
        at = slice(t * LANES, (t + 1) * LANES)
        block = lax.dot_general(
            jnp.ones((8, 2 * LANES), BF16), split_s[at, :], NT, preferred_element_type=F32
        ) / jnp.maximum(block_counts[t], 1.0)
        high = block.astype(BF16).astype(F32)
        middle = (block - high).astype(BF16).astype(F32)
        low = block - high - middle
        piece = jnp.where(sub == 0, high, jnp.where(sub == 1, middle, jnp.where(sub == 2, low, 0.0)))
        pieces.append(piece.astype(BF16))
    blocks = jnp.concatenate(pieces, axis=1)
    for i in range(n_chunks):
        c = jnp.where(my_chunk < n_chunks // 2, n_chunks - 1 - i, i)
        at = pl.ds(pl.multiple_of(c * chunk, chunk), chunk)
        moved = jnp.sum(
            lax.dot_general(blocks, perm_s[at, :], NT, preferred_element_type=F32), axis=0, keepdims=True
        )
        for q in range(group):
            peer = c * group + q
            part = moved[:, q * per_peer : (q + 1) * per_peer]
            bsend_s[peer] = jnp.concatenate(
                [part, jnp.zeros((1, LANES - per_peer), F32)], axis=1
            )

            @pl.when(peer != my_dp)
            def _():
                pltpu.make_async_remote_copy(
                    src_ref=bsend_s.at[peer], dst_ref=brecv_s.at[my_dp], send_sem=blk_send,
                    recv_sem=blk_recv, device_id={"grp": my_grp, "dp": peer}, device_id_type=MESH,
                ).start()

            @pl.when(peer == my_dp)
            def _():
                brecv_s[my_dp] = bsend_s[peer]

    own = send_s.at[pl.ds(0, per_peer)]
    pltpu.make_async_copy(own, tok_out.at[pl.ds(0, per_peer)], own_sem).wait()
    pltpu.make_async_copy(everyone, everyone, st_send).wait()
    others = pl.ds(0, rows - per_peer)
    for sem in (tok_send, tok_recv):
        pltpu.make_async_copy(send_s.at[others], tok_out.at[others], sem).wait()
    peers = bsend_s.at[pl.ds(0, n_dp - 1)]
    for sem in (blk_send, blk_recv):
        pltpu.make_async_copy(peers, peers, sem).wait()
    beside = LANES // per_peer
    for r in range(tiles):
        line = brecv_s[r * beside]
        for q in range(1, beside):
            line = line + pltpu.roll(brecv_s[r * beside + q], q * per_peer, 1)
        blk_out[r : r + 1, :] = line


def finish(tok_ref, blk_ref, tok_out, blk_out, sem):
    copies = [
        pltpu.make_async_copy(tok_ref, tok_out, sem.at[0]),
        pltpu.make_async_copy(blk_ref, blk_out, sem.at[1]),
    ]
    for copy in copies:
        copy.start()
    for copy in copies:
        copy.wait()


def solution(mesh):
    n_grp, n_dp = mesh.shape["grp"], mesh.shape["dp"]

    def on_device(version_tags, packed_pos, valid_mask, returns, values, log_ratio_new, log_ratio_prox):
        rows, width = returns.shape
        n_all = n_grp * n_dp
        per_peer = rows // n_dp
        vmem = pl.BlockSpec(memory_space=pltpu.VMEM)
        anywhere = pl.BlockSpec(memory_space=pl.ANY)
        dma = pltpu.SemaphoreType.DMA
        full = pltpu.VMEM((rows, width), F32)
        token_loss, block_loss = pl.pallas_call(
            functools.partial(kernel, n_grp, n_dp),
            out_shape=(
                pltpu.VMEM((rows, width), F32),
                pltpu.VMEM((rows // LANES, LANES), F32),
            ),
            in_specs=[vmem, vmem] + [anywhere] * 5,
            out_specs=(vmem, vmem),
            scratch_shapes=[
                pltpu.VMEM((rows, width), jnp.int32), full, full, full, full, full,
                pltpu.VMEM((rows, rows), BF16),
                pltpu.VMEM((rows, 2 * width), BF16),
                full,
                pltpu.VMEM((n_dp, 1, width), F32),
                pltpu.VMEM((n_dp, 1, width), F32),
                pltpu.VMEM((n_all, 1, width), F32),
                dma((5,)), dma, dma, dma, dma, dma, dma, dma,
            ],
            compiler_params=pltpu.CompilerParams(collective_id=0, has_side_effects=True),
        )(
            version_tags.reshape(rows // LANES, LANES), packed_pos.reshape(rows // LANES, LANES),
            valid_mask, returns, values, log_ratio_new, log_ratio_prox,
        )
        token_loss, block_loss = pl.pallas_call(
            finish,
            out_shape=(
                jax.ShapeDtypeStruct((rows, width), F32),
                jax.ShapeDtypeStruct((rows // LANES, LANES), F32),
            ),
            in_specs=[anywhere] * 2,
            out_specs=(anywhere, anywhere),
            scratch_shapes=[dma((2,))],
            compiler_params=pltpu.CompilerParams(vmem_limit_bytes=1 << 20),
        )(token_loss, block_loss)
        return token_loss, block_loss.reshape(rows)

    each = P(("grp", "dp"))
    wide = P(("grp", "dp"), None)
    return jax.shard_map(
        on_device, mesh=mesh, in_specs=(each, each) + (wide,) * 5, out_specs=(wide, each), check_vma=False
    )
```

```python
import functools

import jax
import jax.numpy as jnp
from jax import lax
from jax.experimental import pallas as pl
from jax.experimental.pallas import tpu as pltpu
from jax.sharding import PartitionSpec as P

VERSIONS = 4
LANES = 128
F32 = jnp.float32
BF16 = jnp.bfloat16
MESH = pl.DeviceIdType.MESH
NT = (((1,), (1,)), ((), ()))


def fold(array):
    return jnp.sum(array.reshape(-1, 8, array.shape[-1]), axis=0)


def total(array):
    return jnp.sum(jnp.sum(array, axis=0, keepdims=True), axis=1, keepdims=True)


def pick(tags, per_version):
    chosen = per_version[-1]
    for v in range(VERSIONS - 2, -1, -1):
        chosen = jnp.where(tags == v, per_version[v], chosen)
    return chosen


def kernel(
    n_grp, n_dp,
    tags_ref, packed_ref, mask_hbm, ret_hbm, val_hbm, new_hbm, prox_hbm,
    tok_out, blk_out,
    mask_s, ret_s, val_s, new_s, prox_s, tags_s, perm_s, split_s, send_s, bsend_s, brecv_s, stats_s,
    load_sem, st_send, st_recv, tok_send, tok_recv, blk_send, blk_recv, own_sem,
):
    n_all = n_grp * n_dp
    my_grp, my_dp = lax.axis_index("grp"), lax.axis_index("dp")
    me = my_grp * n_dp + my_dp
    rows = ret_s.shape[0]
    tiles = rows // LANES
    per_peer = rows // n_dp
    group = max(1, 256 // per_peer)
    chunk = group * per_peer
    n_chunks = rows // chunk

    place = my_dp * n_grp + my_grp
    low = place < n_all // 2
    mirror = jnp.where(low, n_all - 1 - place, place)

    def device(k):
        step = k - 1 + (k > mirror).astype(jnp.int32)
        index = jnp.where(low, n_all - 1 - step, step)
        return {"grp": lax.rem(index, n_grp), "dp": index // n_grp}

    barrier = pltpu.get_barrier_semaphore()

    @pl.loop(1, n_all, unroll=n_all <= 64)
    def _(k):
        pl.semaphore_signal(
            barrier, inc=1, device_id=device(k), device_id_type=MESH
        )

    loads = [
        pltpu.make_async_copy(src, dst, load_sem.at[i])
        for i, (src, dst) in enumerate(
            ((ret_hbm, ret_s), (val_hbm, val_s), (mask_hbm, mask_s), (new_hbm, new_s), (prox_hbm, prox_s))
        )
    ]
    for load in loads[:3]:
        load.start()

    eye = lax.broadcasted_iota(jnp.int32, (LANES, LANES), 0) == lax.broadcasted_iota(
        jnp.int32, (LANES, LANES), 1
    )
    ones = jnp.ones((LANES, LANES), BF16)
    for t in range(tiles):
        row = tags_ref[t : t + 1, :].astype(F32)
        spread = jnp.where(eye, jnp.broadcast_to(row, (LANES, LANES)), 0.0).astype(BF16)
        tags_s[t * LANES : (t + 1) * LANES, :] = jnp.dot(spread, ones, preferred_element_type=F32)

    for load in loads[:3]:
        load.wait()
    for load in loads[3:]:
        load.start()
    counts = [jnp.zeros((8, LANES), F32)] * VERSIONS
    sums = [jnp.zeros((8, LANES), F32)] * VERSIONS
    for t in range(tiles):
        at = slice(t * LANES, (t + 1) * LANES)
        advantage = ret_s[at, :] - val_s[at, :]
        ret_s[at, :] = advantage
        marked = jnp.where(mask_s[at, :] == 0, -1.0, tags_s[at, :])
        val_s[at, :] = marked
        for v in range(VERSIONS):
            valid = marked == v
            counts[v] = counts[v] + fold(jnp.where(valid, 1.0, 0.0))
            sums[v] = sums[v] + fold(jnp.where(valid, advantage, 0.0))
    counts = [total(c) for c in counts]
    means = [total(s) / jnp.maximum(c, 1.0) for s, c in zip(sums, counts)]
    squares = [jnp.zeros((8, LANES), F32)] * VERSIONS
    for t in range(tiles):
        at = slice(t * LANES, (t + 1) * LANES)
        marked = val_s[at, :]
        advantage = ret_s[at, :]
        for v in range(VERSIONS):
            centered = jnp.where(marked == v, advantage - means[v], 0.0)
            squares[v] = squares[v] + fold(centered * centered)
    squares = [total(s) for s in squares]
    lane = lax.broadcasted_iota(jnp.int32, (1, LANES), 1)
    message = jnp.zeros((1, LANES), F32)
    for i, value in enumerate(counts + means + squares):
        message = jnp.where(lane == i, value, message)
    stats_s[me] = message

    pl.semaphore_wait(barrier, n_all - 1)

    @pl.loop(1, n_all, unroll=n_all <= 64)
    def _(k):
        pltpu.make_async_remote_copy(
            src_ref=stats_s.at[me], dst_ref=stats_s.at[me], send_sem=st_send, recv_sem=st_recv,
            device_id=device(k), device_id_type=MESH,
        ).start()

    base = my_grp * (rows * n_dp) + my_dp * per_peer
    for c in range(n_chunks):
        slot = lax.broadcasted_iota(jnp.int32, (chunk, LANES), 0)
        want = base + (slot // per_peer + c * group) * rows + lax.rem(slot, per_peer)
        for t in range(tiles):
            hit = want == packed_ref[t : t + 1, :]
            perm_s[c * chunk : (c + 1) * chunk, t * LANES : (t + 1) * LANES] = (
                jnp.where(hit, 1.0, 0.0).astype(BF16)
            )
    for load in loads[3:]:
        load.wait()
    block_counts = []
    for t in range(tiles):
        at = slice(t * LANES, (t + 1) * LANES)
        maskf = mask_s[at, :].astype(F32)
        weight = -maskf * jnp.exp(prox_s[at, :])
        ratio = jnp.exp(new_s[at, :])
        new_s[at, :] = weight * ratio
        prox_s[at, :] = weight * jnp.clip(ratio, 0.8, 1.2)
        block_counts.append(
            lax.dot_general(ones[:8], maskf.astype(BF16), NT, preferred_element_type=F32)
        )

    my_chunk = my_dp // group
    blocks = jnp.concatenate(block_counts, axis=1).astype(BF16)
    for i in range(n_chunks):
        c = jnp.where(my_chunk < n_chunks // 2, n_chunks - 1 - i, i)
        at = pl.ds(pl.multiple_of(c * chunk, chunk), chunk)
        moved = lax.dot_general(blocks, perm_s[at, :], NT, preferred_element_type=F32)[:1]
        for q in range(group):
            peer = c * group + q
            part = moved[:, q * per_peer : (q + 1) * per_peer]
            bsend_s[peer] = jnp.concatenate(
                [part, jnp.zeros((1, LANES - per_peer), F32)], axis=1
            )

            @pl.when(peer != my_dp)
            def _():
                pltpu.make_async_remote_copy(
                    src_ref=bsend_s.at[peer], dst_ref=brecv_s.at[my_dp], send_sem=blk_send,
                    recv_sem=blk_recv, device_id={"grp": my_grp, "dp": peer}, device_id_type=MESH,
                ).start()

            @pl.when(peer == my_dp)
            def _():
                brecv_s[my_dp] = bsend_s[peer]

    everyone = stats_s.at[pl.ds(0, n_all - 1)]
    pltpu.make_async_copy(everyone, everyone, st_recv).wait()
    every_count = stats_s[...]
    every_mean = pltpu.roll(every_count, LANES - VERSIONS, 2)
    every_square = pltpu.roll(every_count, LANES - 2 * VERSIONS, 2)
    total_count = jnp.maximum(jnp.sum(every_count, axis=0), 1.0)
    mean_row = jnp.sum(every_count * every_mean, axis=0) / total_count
    off = every_mean - mean_row[None]
    square_row = jnp.sum(every_square + every_count * off * off, axis=0)
    scale_row = 1.0 / jnp.sqrt(square_row / total_count + 0.05)
    means = [mean_row[:, v : v + 1] for v in range(VERSIONS)]
    scales = [scale_row[:, v : v + 1] for v in range(VERSIONS)]

    for t in range(tiles):
        at = slice(t * LANES, (t + 1) * LANES)
        tags = tags_s[at, :]
        white = (ret_s[at, :] - pick(tags, means)) * pick(tags, scales)
        loss = jnp.maximum(new_s[at, :] * white, prox_s[at, :] * white)
        high = loss.astype(BF16)
        split_s[at, :LANES] = high
        split_s[at, LANES:] = (loss - high.astype(F32)).astype(BF16)

    for i in range(n_chunks):
        c = jnp.where(my_chunk < n_chunks // 2, n_chunks - 1 - i, i)
        at = pl.ds(pl.multiple_of(c * chunk, chunk), chunk)
        parts = jnp.dot(perm_s[at, :], split_s[...], preferred_element_type=F32)
        send_s[at, :] = parts[:, :LANES] + parts[:, LANES:]
        for q in range(group):
            peer = c * group + q
            src = send_s.at[pl.ds(pl.multiple_of(peer * per_peer, per_peer), per_peer)]
            dst = tok_out.at[pl.ds(pl.multiple_of(my_dp * per_peer, per_peer), per_peer)]

            @pl.when(peer != my_dp)
            def _():
                pltpu.make_async_remote_copy(
                    src_ref=src, dst_ref=dst, send_sem=tok_send, recv_sem=tok_recv,
                    device_id={"grp": my_grp, "dp": peer}, device_id_type=MESH,
                ).start()

            @pl.when(peer == my_dp)
            def _():
                pltpu.make_async_copy(src, dst, own_sem).start()

    own = send_s.at[pl.ds(0, per_peer)]
    pltpu.make_async_copy(own, tok_out.at[pl.ds(0, per_peer)], own_sem).wait()
    pltpu.make_async_copy(everyone, everyone, st_send).wait()
    others = pl.ds(0, rows - per_peer)
    for sem in (tok_send, tok_recv):
        pltpu.make_async_copy(send_s.at[others], tok_out.at[others], sem).wait()
    peers = bsend_s.at[pl.ds(0, n_dp - 1)]
    for sem in (blk_send, blk_recv):
        pltpu.make_async_copy(peers, peers, sem).wait()
    beside = LANES // per_peer
    for r in range(tiles):
        line = brecv_s[r * beside]
        for q in range(1, beside):
            line = line + pltpu.roll(brecv_s[r * beside + q], q * per_peer, 1)
        rows_in = tok_out[r * LANES : (r + 1) * LANES, :]
        high = rows_in.astype(BF16)
        low = (rows_in - high.astype(F32)).astype(BF16)
        added = lax.dot_general(ones[:8], high, NT, preferred_element_type=F32) + lax.dot_general(
            ones[:8], low, NT, preferred_element_type=F32
        )
        blk_out[r : r + 1, :] = added[:1] / jnp.maximum(line, 1.0)


def finish(tok_ref, blk_ref, tok_out, blk_out, sem):
    copies = [
        pltpu.make_async_copy(tok_ref, tok_out, sem.at[0]),
        pltpu.make_async_copy(blk_ref, blk_out, sem.at[1]),
    ]
    for copy in copies:
        copy.start()
    for copy in copies:
        copy.wait()


def solution(mesh):
    n_grp, n_dp = mesh.shape["grp"], mesh.shape["dp"]

    def on_device(version_tags, packed_pos, valid_mask, returns, values, log_ratio_new, log_ratio_prox):
        rows, width = returns.shape
        n_all = n_grp * n_dp
        per_peer = rows // n_dp
        vmem = pl.BlockSpec(memory_space=pltpu.VMEM)
        anywhere = pl.BlockSpec(memory_space=pl.ANY)
        dma = pltpu.SemaphoreType.DMA
        full = pltpu.VMEM((rows, width), F32)
        token_loss, block_loss = pl.pallas_call(
            functools.partial(kernel, n_grp, n_dp),
            out_shape=(
                pltpu.VMEM((rows, width), F32),
                pltpu.VMEM((rows // LANES, LANES), F32),
            ),
            in_specs=[vmem, vmem] + [anywhere] * 5,
            out_specs=(vmem, vmem),
            scratch_shapes=[
                pltpu.VMEM((rows, width), jnp.int32), full, full, full, full, full,
                pltpu.VMEM((rows, rows), BF16),
                pltpu.VMEM((rows, 2 * width), BF16),
                full,
                pltpu.VMEM((n_dp, 1, width), F32),
                pltpu.VMEM((n_dp, 1, width), F32),
                pltpu.VMEM((n_all, 1, width), F32),
                dma((5,)), dma, dma, dma, dma, dma, dma, dma,
            ],
            compiler_params=pltpu.CompilerParams(collective_id=0, has_side_effects=True),
        )(
            version_tags.reshape(rows // LANES, LANES), packed_pos.reshape(rows // LANES, LANES),
            valid_mask, returns, values, log_ratio_new, log_ratio_prox,
        )
        token_loss, block_loss = pl.pallas_call(
            finish,
            out_shape=(
                jax.ShapeDtypeStruct((rows, width), F32),
                jax.ShapeDtypeStruct((rows // LANES, LANES), F32),
            ),
            in_specs=[anywhere] * 2,
            out_specs=(anywhere, anywhere),
            scratch_shapes=[dma((2,))],
            compiler_params=pltpu.CompilerParams(vmem_limit_bytes=1 << 20),
        )(token_loss, block_loss)
        return token_loss, block_loss.reshape(rows)

    each = P(("grp", "dp"))
    wide = P(("grp", "dp"), None)
    return jax.shard_map(
        on_device, mesh=mesh, in_specs=(each, each) + (wide,) * 5, out_specs=(wide, each), check_vma=False
    )
```

```python
import functools

import jax
import jax.numpy as jnp
from jax import lax
from jax.experimental import pallas as pl
from jax.experimental.pallas import tpu as pltpu
from jax.sharding import PartitionSpec as P

VERSIONS = 4
LANES = 128
F32 = jnp.float32
BF16 = jnp.bfloat16
MESH = pl.DeviceIdType.MESH
NT = (((1,), (1,)), ((), ()))


def fold(array):
    return jnp.sum(array.reshape(-1, 8, array.shape[-1]), axis=0)


def total(array):
    return jnp.sum(jnp.sum(array, axis=0, keepdims=True), axis=1, keepdims=True)


def pick(tags, per_version):
    chosen = per_version[-1]
    for v in range(VERSIONS - 2, -1, -1):
        chosen = jnp.where(tags == v, per_version[v], chosen)
    return chosen


def kernel(
    n_grp, n_dp,
    tags_ref, packed_ref, mask_hbm, ret_hbm, val_hbm, new_hbm, prox_hbm,
    tok_out, blk_out,
    mask_s, ret_s, val_s, new_s, prox_s, tags_s, perm_s, split_s, send_s, bsend_s, brecv_s, stats_s,
    load_sem, st_send, st_recv, tok_send, tok_recv, blk_send, blk_recv, own_sem,
):
    n_all = n_grp * n_dp
    my_grp, my_dp = lax.axis_index("grp"), lax.axis_index("dp")
    me = my_grp * n_dp + my_dp
    rows = ret_s.shape[0]
    tiles = rows // LANES
    per_peer = rows // n_dp
    group = max(1, 128 // per_peer)
    chunk = group * per_peer
    n_chunks = rows // chunk

    place = my_dp * n_grp + my_grp
    low = place < n_all // 2
    mirror = jnp.where(low, n_all - 1 - place, place)

    def device(k):
        step = k - 1 + (k > mirror).astype(jnp.int32)
        index = jnp.where(low, n_all - 1 - step, step)
        return {"grp": lax.rem(index, n_grp), "dp": index // n_grp}

    barrier = pltpu.get_barrier_semaphore()

    @pl.loop(1, n_all, unroll=n_all <= 64)
    def _(k):
        pl.semaphore_signal(
            barrier, inc=1, device_id=device(k), device_id_type=MESH
        )

    loads = [
        pltpu.make_async_copy(src, dst, load_sem.at[i])
        for i, (src, dst) in enumerate(
            ((ret_hbm, ret_s), (val_hbm, val_s), (mask_hbm, mask_s), (new_hbm, new_s), (prox_hbm, prox_s))
        )
    ]
    for load in loads[:3]:
        load.start()

    eye = lax.broadcasted_iota(jnp.int32, (LANES, LANES), 0) == lax.broadcasted_iota(
        jnp.int32, (LANES, LANES), 1
    )
    ones = jnp.ones((LANES, LANES), BF16)
    for t in range(tiles):
        row = tags_ref[t : t + 1, :].astype(F32)
        spread = jnp.where(eye, jnp.broadcast_to(row, (LANES, LANES)), 0.0).astype(BF16)
        tags_s[t * LANES : (t + 1) * LANES, :] = jnp.dot(spread, ones, preferred_element_type=F32)

    for load in loads[:3]:
        load.wait()
    for load in loads[3:]:
        load.start()
    counts = [jnp.zeros((8, LANES), F32)] * VERSIONS
    sums = [jnp.zeros((8, LANES), F32)] * VERSIONS
    for t in range(tiles):
        at = slice(t * LANES, (t + 1) * LANES)
        advantage = ret_s[at, :] - val_s[at, :]
        ret_s[at, :] = advantage
        marked = jnp.where(mask_s[at, :] == 0, -1.0, tags_s[at, :])
        val_s[at, :] = marked
        for v in range(VERSIONS):
            valid = marked == v
            counts[v] = counts[v] + fold(jnp.where(valid, 1.0, 0.0))
            sums[v] = sums[v] + fold(jnp.where(valid, advantage, 0.0))
    counts = [total(c) for c in counts]
    means = [total(s) / jnp.maximum(c, 1.0) for s, c in zip(sums, counts)]
    squares = [jnp.zeros((8, LANES), F32)] * VERSIONS
    for t in range(tiles):
        at = slice(t * LANES, (t + 1) * LANES)
        marked = val_s[at, :]
        advantage = ret_s[at, :]
        for v in range(VERSIONS):
            centered = jnp.where(marked == v, advantage - means[v], 0.0)
            squares[v] = squares[v] + fold(centered * centered)
    squares = [total(s) for s in squares]
    lane = lax.broadcasted_iota(jnp.int32, (1, LANES), 1)
    message = jnp.zeros((1, LANES), F32)
    for i, value in enumerate(counts + means + squares):
        message = jnp.where(lane == i, value, message)
    stats_s[me] = message

    pl.semaphore_wait(barrier, n_all - 1)

    @pl.loop(1, n_all, unroll=n_all <= 64)
    def _(k):
        pltpu.make_async_remote_copy(
            src_ref=stats_s.at[me], dst_ref=stats_s.at[me], send_sem=st_send, recv_sem=st_recv,
            device_id=device(k), device_id_type=MESH,
        ).start()

    base = my_grp * (rows * n_dp) + my_dp * per_peer
    for c in range(n_chunks):
        slot = lax.broadcasted_iota(jnp.int32, (chunk, LANES), 0)
        want = base + (slot // per_peer + c * group) * rows + lax.rem(slot, per_peer)
        for t in range(tiles):
            hit = want == packed_ref[t : t + 1, :]
            perm_s[c * chunk : (c + 1) * chunk, t * LANES : (t + 1) * LANES] = (
                jnp.where(hit, 1.0, 0.0).astype(BF16)
            )
    for load in loads[3:]:
        load.wait()
    block_counts = []
    for t in range(tiles):
        at = slice(t * LANES, (t + 1) * LANES)
        maskf = mask_s[at, :].astype(F32)
        weight = -maskf * jnp.exp(prox_s[at, :])
        ratio = jnp.exp(new_s[at, :])
        new_s[at, :] = weight * ratio
        prox_s[at, :] = weight * jnp.clip(ratio, 0.8, 1.2)
        block_counts.append(
            lax.dot_general(ones[:8], maskf.astype(BF16), NT, preferred_element_type=F32)
        )

    my_chunk = my_dp // group
    blocks = jnp.concatenate(block_counts, axis=1).astype(BF16)
    for i in range(n_chunks):
        c = jnp.where(my_chunk < n_chunks // 2, n_chunks - 1 - i, i)
        at = pl.ds(pl.multiple_of(c * chunk, chunk), chunk)
        moved = lax.dot_general(blocks, perm_s[at, :], NT, preferred_element_type=F32)[:1]
        for q in range(group):
            peer = c * group + q
            part = moved[:, q * per_peer : (q + 1) * per_peer]
            bsend_s[peer] = jnp.concatenate(
                [part, jnp.zeros((1, LANES - per_peer), F32)], axis=1
            )

            @pl.when(peer != my_dp)
            def _():
                pltpu.make_async_remote_copy(
                    src_ref=bsend_s.at[peer], dst_ref=brecv_s.at[my_dp], send_sem=blk_send,
                    recv_sem=blk_recv, device_id={"grp": my_grp, "dp": peer}, device_id_type=MESH,
                ).start()

            @pl.when(peer == my_dp)
            def _():
                brecv_s[my_dp] = bsend_s[peer]

    everyone = stats_s.at[pl.ds(0, n_all - 1)]
    pltpu.make_async_copy(everyone, everyone, st_recv).wait()
    every_count = stats_s[...]
    every_mean = pltpu.roll(every_count, LANES - VERSIONS, 2)
    every_square = pltpu.roll(every_count, LANES - 2 * VERSIONS, 2)
    total_count = jnp.maximum(jnp.sum(every_count, axis=0), 1.0)
    mean_row = jnp.sum(every_count * every_mean, axis=0) / total_count
    off = every_mean - mean_row[None]
    square_row = jnp.sum(every_square + every_count * off * off, axis=0)
    scale_row = 1.0 / jnp.sqrt(square_row / total_count + 0.05)
    means = [mean_row[:, v : v + 1] for v in range(VERSIONS)]
    scales = [scale_row[:, v : v + 1] for v in range(VERSIONS)]

    for t in range(tiles):
        at = slice(t * LANES, (t + 1) * LANES)
        tags = tags_s[at, :]
        white = (ret_s[at, :] - pick(tags, means)) * pick(tags, scales)
        loss = jnp.maximum(new_s[at, :] * white, prox_s[at, :] * white)
        high = loss.astype(BF16)
        split_s[at, :LANES] = high
        split_s[at, LANES:] = (loss - high.astype(F32)).astype(BF16)

    for i in range(n_chunks):
        c = jnp.where(my_chunk < n_chunks // 2, n_chunks - 1 - i, i)
        at = pl.ds(pl.multiple_of(c * chunk, chunk), chunk)
        parts = jnp.dot(perm_s[at, :], split_s[...], preferred_element_type=F32)
        send_s[at, :] = parts[:, :LANES] + parts[:, LANES:]
        for q in range(group):
            peer = c * group + q
            src = send_s.at[pl.ds(pl.multiple_of(peer * per_peer, per_peer), per_peer)]
            dst = tok_out.at[pl.ds(pl.multiple_of(my_dp * per_peer, per_peer), per_peer)]

            @pl.when(peer != my_dp)
            def _():
                pltpu.make_async_remote_copy(
                    src_ref=src, dst_ref=dst, send_sem=tok_send, recv_sem=tok_recv,
                    device_id={"grp": my_grp, "dp": peer}, device_id_type=MESH,
                ).start()

            @pl.when(peer == my_dp)
            def _():
                pltpu.make_async_copy(src, dst, own_sem).start()

    own = send_s.at[pl.ds(0, per_peer)]
    pltpu.make_async_copy(own, tok_out.at[pl.ds(0, per_peer)], own_sem).wait()
    pltpu.make_async_copy(everyone, everyone, st_send).wait()
    others = pl.ds(0, rows - per_peer)
    for sem in (tok_send, tok_recv):
        pltpu.make_async_copy(send_s.at[others], tok_out.at[others], sem).wait()
    peers = bsend_s.at[pl.ds(0, n_dp - 1)]
    for sem in (blk_send, blk_recv):
        pltpu.make_async_copy(peers, peers, sem).wait()
    beside = LANES // per_peer
    for r in range(tiles):
        line = brecv_s[r * beside]
        for q in range(1, beside):
            line = line + pltpu.roll(brecv_s[r * beside + q], q * per_peer, 1)
        rows_in = tok_out[r * LANES : (r + 1) * LANES, :]
        high = rows_in.astype(BF16)
        low = (rows_in - high.astype(F32)).astype(BF16)
        added = lax.dot_general(ones[:8], high, NT, preferred_element_type=F32) + lax.dot_general(
            ones[:8], low, NT, preferred_element_type=F32
        )
        blk_out[r : r + 1, :] = added[:1] / jnp.maximum(line, 1.0)


def finish(tok_ref, blk_ref, tok_out, blk_out, sem):
    copies = [
        pltpu.make_async_copy(tok_ref, tok_out, sem.at[0]),
        pltpu.make_async_copy(blk_ref, blk_out, sem.at[1]),
    ]
    for copy in copies:
        copy.start()
    for copy in copies:
        copy.wait()


def solution(mesh):
    n_grp, n_dp = mesh.shape["grp"], mesh.shape["dp"]

    def on_device(version_tags, packed_pos, valid_mask, returns, values, log_ratio_new, log_ratio_prox):
        rows, width = returns.shape
        n_all = n_grp * n_dp
        per_peer = rows // n_dp
        vmem = pl.BlockSpec(memory_space=pltpu.VMEM)
        anywhere = pl.BlockSpec(memory_space=pl.ANY)
        dma = pltpu.SemaphoreType.DMA
        full = pltpu.VMEM((rows, width), F32)
        token_loss, block_loss = pl.pallas_call(
            functools.partial(kernel, n_grp, n_dp),
            out_shape=(
                pltpu.VMEM((rows, width), F32),
                pltpu.VMEM((rows // LANES, LANES), F32),
            ),
            in_specs=[vmem, vmem] + [anywhere] * 5,
            out_specs=(vmem, vmem),
            scratch_shapes=[
                pltpu.VMEM((rows, width), jnp.int32), full, full, full, full, full,
                pltpu.VMEM((rows, rows), BF16),
                pltpu.VMEM((rows, 2 * width), BF16),
                full,
                pltpu.VMEM((n_dp, 1, width), F32),
                pltpu.VMEM((n_dp, 1, width), F32),
                pltpu.VMEM((n_all, 1, width), F32),
                dma((5,)), dma, dma, dma, dma, dma, dma, dma,
            ],
            compiler_params=pltpu.CompilerParams(collective_id=0, has_side_effects=True),
        )(
            version_tags.reshape(rows // LANES, LANES), packed_pos.reshape(rows // LANES, LANES),
            valid_mask, returns, values, log_ratio_new, log_ratio_prox,
        )
        token_loss, block_loss = pl.pallas_call(
            finish,
            out_shape=(
                jax.ShapeDtypeStruct((rows, width), F32),
                jax.ShapeDtypeStruct((rows // LANES, LANES), F32),
            ),
            in_specs=[anywhere] * 2,
            out_specs=(anywhere, anywhere),
            scratch_shapes=[dma((2,))],
            compiler_params=pltpu.CompilerParams(vmem_limit_bytes=1 << 20),
        )(token_loss, block_loss)
        return token_loss, block_loss.reshape(rows)

    each = P(("grp", "dp"))
    wide = P(("grp", "dp"), None)
    return jax.shard_map(
        on_device, mesh=mesh, in_specs=(each, each) + (wide,) * 5, out_specs=(wide, each), check_vma=False
    )
```
